32 devices in a mesh: shot: 4 (over y, core), tile: 8 (over z, x).
Axes of the slice: x: 2, y: 2, z: 4, core: 2. Of those that a mesh axis runs over, the one named last changes fastest.
Arguments:
- source: bfloat16 [64, 1, 32, 32, 128], P(('shot', 'tile')), may hold values from -6 to 6
- receiver: bfloat16 [64, 1, 32, 32, 128], P(('shot', 'tile')), may hold values from -6 to 6
- corners: int32 [64, 2], P(('shot', 'tile')), may hold values from 0 to 224, as said below
Outputs:
- filtered: float32 [32, 256, 256], P('tile', 'shot')
The draws below stay inside these ranges and needn't reach their ends.
Inputs may be any that keep to these rules, and one draw needn't show every extreme that they name: corners[s, 0] is at most 224 and corners[s, 1] at most 128, so every box lies inside the image.
All inputs are finite; a program needn't handle non-finite values.
Results may differ from the reference program's by a relative error of at most 0.0003.
Values may be sent and summed in bfloat16 or wider, within the bound.
A program may use at most 64 MiB of HBM per device.

```python
import jax
import jax.numpy as jnp
from jax import lax

NT = 1
X = 256
Y = 256
BX = 32
BY = 128
SHOTS = 64
Z = 32


def draw_corners(key, part):
    first_key, second_key = jax.random.split(jax.random.fold_in(key, 17))
    row_start = jax.random.randint(first_key, (SHOTS, 1), 0, X - BX + 1)
    col_start = jax.random.randint(second_key, (SHOTS, 1), 0, Y - BY + 1)
    return jnp.concatenate((row_start, col_start), axis=1).astype(jnp.int32)


def level_of(stream_key, dims, cuts, least, largest):
    factor_of = 1.0
    for axis_at, shards_of in cuts:
        steps = jax.random.uniform(jax.random.fold_in(jax.random.fold_in(stream_key, 6), axis_at), (shards_of,), jnp.float32, least / len(cuts), largest / len(cuts))
        factor_of = factor_of * jnp.repeat(jnp.exp(steps), dims[axis_at] // shards_of).reshape((-1,) + (1,) * (len(dims) - 1 - axis_at))
    return factor_of


def bell_draw(key, dims, spread, reach, cuts=(), kind=jnp.bfloat16):
    result = jax.random.normal(key, dims, jnp.float32) * spread
    if len(cuts) > 0:
        result = level_of(key, dims, cuts, -0.22, 0.18) * result
    return jnp.clip(result, min=-reach, max=reach).astype(kind)


def setup_inputs(seed: int = 0) -> dict:
    keys = jax.random.split(jax.random.key(seed), 4)
    return {
        "source": bell_draw(keys[0], (SHOTS, NT, Z, BX, BY), 1.0, 6.0, ((0, 32),)),
        "receiver": bell_draw(keys[1], (SHOTS, NT, Z, BX, BY), 1.0, 6.0, ((0, 32),)),
        "corners": draw_corners(jax.random.fold_in(keys[3], 71), 0),
    }


damping = 1.0


def reference(source, receiver, corners):
    def place(shot, totals):
        image, lights = totals
        wave = lax.dynamic_index_in_dim(source, shot, 0, keepdims=False).astype(jnp.float32)
        back = lax.dynamic_index_in_dim(receiver, shot, 0, keepdims=False).astype(jnp.float32)
        partial_value = jnp.sum(wave * back, axis=0)
        light = jnp.sum(wave * wave, axis=0)
        start = (jnp.int32(0), corners[shot, 0].astype(jnp.int32), corners[shot, 1].astype(jnp.int32))
        image = lax.dynamic_update_slice(image, lax.dynamic_slice(image, start, (Z, BX, BY)) + partial_value, start)
        lights = lax.dynamic_update_slice(lights, lax.dynamic_slice(lights, start, (Z, BX, BY)) + light, start)
        return image, lights

    empty = jnp.zeros((Z, X, Y), jnp.float32)
    image, lights = lax.fori_loop(0, SHOTS, place, (empty, empty))
    normal = image / (damping + lights)
    padded = jnp.pad(normal, 1)
    beside = padded[2:, 1:-1, 1:-1] + padded[:-2, 1:-1, 1:-1]
    beside = beside + padded[1:-1, 2:, 1:-1] + padded[1:-1, :-2, 1:-1]
    beside = beside + padded[1:-1, 1:-1, 2:] + padded[1:-1, 1:-1, :-2]
    return beside - 6.0 * normal
```

```python
import functools

import jax
import jax.numpy as jnp
from jax import lax
from jax.experimental import pallas as pl
from jax.experimental.pallas import tpu as pltpu
from jax.sharding import PartitionSpec as P

X = 256
Y = 256
LANES = 128

damping = 1.0


def kernel(
    ns, nt, src, rcv, cor, out, rx, cbuf, csm, boxes, acc, r1, r2, nrm, hx, hz, rows,
    rx_send, rx_recv, c_send, c_recv, c_local, s1_send, s1_recv, s2_send, s2_recv, h_send, h_recv,
):
    depth, strip, width = nrm.shape
    spd, samples = src.shape[0], src.shape[1]
    box_rows = src.shape[3]
    halves = width // LANES
    shots = nt * spd
    block = min(box_rows, strip)
    per_strip = strip // block
    half_ns = ns // 2
    shot = lax.axis_index("shot")
    tile = lax.axis_index("tile")
    core = lax.rem(shot, 2)
    pair = shot // 2
    other = 1 - core

    barrier = pltpu.get_barrier_semaphore()
    for k in range(1, ns):
        pl.semaphore_signal(barrier, inc=1, device_id={"shot": lax.rem(shot + k, ns)})
    for k in range(1, nt):
        pl.semaphore_signal(barrier, inc=1, device_id={"tile": lax.rem(tile + k, nt)})

    own = []
    for p in range(depth):
        for w, ref in enumerate((src, rcv)):
            copy = pltpu.make_async_copy(ref.at[:, :, tile * depth + p], rx.at[p, tile, w], rx_recv.at[p])
            copy.start()
    own_corner = pltpu.make_async_copy(cor, cbuf.at[tile], c_recv)
    own_corner.start()

    pl.semaphore_wait(barrier, ns - 1 + nt - 1)

    for k in range(1, nt):
        to = lax.rem(tile + k, nt)
        pltpu.make_async_remote_copy(
            src_ref=cor, dst_ref=cbuf.at[tile], send_sem=c_send, recv_sem=c_recv, device_id={"tile": to}
        ).start()
    for p in range(depth):
        for k in range(1, nt):
            to = lax.rem(tile + k, nt)
            for w, ref in enumerate((src, rcv)):
                pltpu.make_async_remote_copy(
                    src_ref=ref.at[:, :, to * depth + p],
                    dst_ref=rx.at[p, tile, w],
                    send_sem=rx_send.at[p],
                    recv_sem=rx_recv.at[p],
                    device_id={"tile": to},
                ).start()

    zero = jnp.zeros((block, LANES), jnp.float32)

    def clear(s, carry):
        for q in range(2):
            for h in range(halves):
                boxes[s, q, h, pl.ds(0, block), :] = zero
                boxes[s, q, h, pl.ds(block + box_rows, block), :] = zero
        return carry

    lax.fori_loop(0, shots, clear, 0)

    pltpu.make_async_copy(cbuf, cbuf, c_recv).wait()
    to_scalar = pltpu.make_async_copy(cbuf, csm, c_local)
    to_scalar.start()
    to_scalar.wait()

    lane = lax.broadcasted_iota(jnp.int32, (box_rows, LANES), 1)

    def expand(p):
        def peer(t, carry):
            for i in range(spd):
                s = t * spd + i
                col = csm[t, i, 1]
                turn = lax.rem(col, LANES)
                image = jnp.zeros((box_rows, LANES), jnp.float32)
                light = image
                for n in range(samples):
                    wave = rx[p, t, 0, i, n].astype(jnp.float32)
                    back = rx[p, t, 1, i, n].astype(jnp.float32)
                    image = wave * back if n == 0 else image + wave * back
                    light = wave * wave if n == 0 else light + wave * wave
                image = pltpu.roll(image, turn, 1)
                light = pltpu.roll(light, turn, 1)
                for h in range(halves):
                    at = lane + (h * LANES - col)
                    inside = (at >= 0) & (at < LANES)
                    boxes[s, 0, h, pl.ds(block, box_rows), :] = jnp.where(inside, image, 0.0)
                    boxes[s, 1, h, pl.ds(block, box_rows), :] = jnp.where(inside, light, 0.0)
            return carry

        lax.fori_loop(0, nt, peer, 0)

    def place(p, parity):
        def one(n, carry):
            j = 2 * (n // per_strip) + parity
            base = lax.rem(n, per_strip) * block
            first = j * strip + base + block
            total = [[None] * halves for _ in range(2)]
            for s in range(shots):
                start = jnp.clip(first - csm[s // spd, s % spd, 0], 0, box_rows + block)
                for q in range(2):
                    for h in range(halves):
                        piece = boxes[s, q, h, pl.ds(start, block), :]
                        total[q][h] = piece if s == 0 else total[q][h] + piece
            for q in range(2):
                for h in range(halves):
                    acc[p, j, q, pl.ds(base, block), pl.ds(h * LANES, LANES)] = total[q][h]
            return carry

        lax.fori_loop(0, half_ns * per_strip, one, 0)

    def stage1(p):
        for i in range(half_ns):
            pltpu.make_async_remote_copy(
                src_ref=acc.at[p, 2 * i + other],
                dst_ref=r1.at[p, i],
                send_sem=s1_send.at[p],
                recv_sem=s1_recv.at[p],
                device_id={"shot": 2 * pair + other},
            ).start()

    def stage2(p):
        pltpu.make_async_copy(r1.at[p], r1.at[p], s1_recv.at[p]).wait()
        for k in range(1, half_ns):
            to = lax.rem(pair + k, half_ns)
            j = 2 * to + core
            acc[p, j] = acc[p, j] + r1[p, to]
            pltpu.make_async_remote_copy(
                src_ref=acc.at[p, j],
                dst_ref=r2.at[p, k - 1],
                send_sem=s2_send.at[p],
                recv_sem=s2_recv.at[p],
                device_id={"shot": j},
            ).start()

    def finish(p):
        pltpu.make_async_copy(r2.at[p], r2.at[p], s2_recv.at[p]).wait()
        image = acc[p, shot, 0] + r1[p, pair, 0]
        light = acc[p, shot, 1] + r1[p, pair, 1]
        for k in range(half_ns - 1):
            image = image + r2[p, k, 0]
            light = light + r2[p, k, 1]
        normal = image / (damping + light)
        nrm[p] = normal
        rows[0, pl.ds(p, 1), :] = normal[strip - 1 :, :]
        rows[1, pl.ds(p, 1), :] = normal[:1, :]

    for p in range(depth):
        pltpu.make_async_copy(rx.at[p], rx.at[p], rx_recv.at[p]).wait()
        expand(p)
        place(p, other)
        stage1(p)
        place(p, core)
        if p >= 1:
            stage2(p - 1)
        if p >= 2:
            finish(p - 2)
    stage2(depth - 1)
    if depth >= 2:
        finish(depth - 2)
    finish(depth - 1)

    halos = (
        (shot < ns - 1, shot > 0, {"shot": lax.rem(shot + 1, ns)}, rows.at[0], hx.at[0], 0),
        (shot > 0, shot < ns - 1, {"shot": lax.rem(shot + ns - 1, ns)}, rows.at[1], hx.at[1], 1),
        (tile < nt - 1, tile > 0, {"tile": lax.rem(tile + 1, nt)}, nrm.at[depth - 1], hz.at[0], 2),
        (tile > 0, tile < nt - 1, {"tile": lax.rem(tile + nt - 1, nt)}, nrm.at[0], hz.at[1], 3),
    )

    def halo_copy(item):
        return pltpu.make_async_remote_copy(
            src_ref=item[3], dst_ref=item[4], send_sem=h_send.at[item[5]], recv_sem=h_recv.at[item[5]], device_id=item[2]
        )

    for item in halos:
        @pl.when(item[0])
        def _(item=item):
            halo_copy(item).start()

        @pl.when(jnp.logical_not(item[1]))
        def _(item=item):
            item[4][...] = jnp.zeros(item[4].shape, jnp.float32)

    for item in halos:
        @pl.when(item[1])
        def _(item=item):
            halo_copy(item).wait_recv()

    row = lax.broadcasted_iota(jnp.int32, (strip, width), 0)
    column = lax.broadcasted_iota(jnp.int32, (strip, width), 1)
    for p in range(depth):
        center = nrm[p]
        above = nrm[p - 1] if p > 0 else hz[0]
        below = nrm[p + 1] if p < depth - 1 else hz[1]
        beside = above + below
        before = jnp.where(row == 0, hx[0, pl.ds(p, 1), :], pltpu.roll(center, 1, 0))
        after = jnp.where(row == strip - 1, hx[1, pl.ds(p, 1), :], pltpu.roll(center, strip - 1, 0))
        beside = beside + before + after
        left = jnp.where(column == 0, 0.0, pltpu.roll(center, 1, 1))
        right = jnp.where(column == width - 1, 0.0, pltpu.roll(center, width - 1, 1))
        beside = beside + left + right
        out[p] = beside - 6.0 * center

    for item in halos:
        @pl.when(item[0])
        def _(item=item):
            halo_copy(item).wait_send()

    sent = cbuf.at[pl.ds(0, nt - 1)]
    pltpu.make_async_copy(sent, sent, c_send).wait()
    for p in range(depth):
        sent = rx.at[p, pl.ds(0, nt - 1)]
        pltpu.make_async_copy(sent, sent, rx_send.at[p]).wait()
        pltpu.make_async_copy(r1.at[p], r1.at[p], s1_send.at[p]).wait()
        pltpu.make_async_copy(r2.at[p], r2.at[p], s2_send.at[p]).wait()


def solution(mesh):
    ns, nt = mesh.shape["shot"], mesh.shape["tile"]

    def step(source, receiver, corners):
        spd, samples, full_depth, box_rows, box_cols = source.shape
        depth = full_depth // nt
        strip = X // ns
        block = min(box_rows, strip)
        half_ns = ns // 2
        vmem = pltpu.VMEM
        dma = pltpu.SemaphoreType.DMA
        f32 = jnp.float32
        return pl.pallas_call(
            functools.partial(kernel, ns, nt),
            out_shape=jax.ShapeDtypeStruct((depth, strip, Y), f32),
            in_specs=[pl.BlockSpec(memory_space=pl.ANY)] * 3,
            out_specs=pl.BlockSpec(memory_space=pltpu.VMEM),
            scratch_shapes=[
                vmem((depth, nt, 2, spd, samples, box_rows, box_cols), jnp.bfloat16),
                vmem((nt, spd, 2), jnp.int32),
                pltpu.SMEM((nt, spd, 2), jnp.int32),
                vmem((nt * spd, 2, Y // LANES, box_rows + 2 * block, LANES), f32),
                vmem((depth, ns, 2, strip, Y), f32),
                vmem((depth, half_ns, 2, strip, Y), f32),
                vmem((depth, half_ns - 1, 2, strip, Y), f32),
                vmem((depth, strip, Y), f32),
                vmem((2, depth, Y), f32),
                vmem((2, strip, Y), f32),
                vmem((2, depth, Y), f32),
                dma((depth,)),
                dma((depth,)),
                dma,
                dma,
                dma,
                dma((depth,)),
                dma((depth,)),
                dma((depth,)),
                dma((depth,)),
                dma((4,)),
                dma((4,)),
            ],
            compiler_params=pltpu.CompilerParams(
                collective_id=0, has_side_effects=True, vmem_limit_bytes=60 * 1024 * 1024
            ),
        )(source, receiver, corners)

    return jax.shard_map(
        step,
        mesh=mesh,
        in_specs=(
            P(("shot", "tile"), None, None, None, None),
            P(("shot", "tile"), None, None, None, None),
            P(("shot", "tile"), None),
        ),
        out_specs=P("tile", "shot", None),
        check_vma=False,
    )
```

```python
import functools

import jax
import jax.numpy as jnp
from jax import lax
from jax.experimental import pallas as pl
from jax.experimental.pallas import tpu as pltpu
from jax.sharding import PartitionSpec as P

X = 256
Y = 256
LANES = 128

damping = 1.0


def partner(index, k, count):
    if count & (count - 1):
        return lax.rem(index + k, count)
    bit = 1
    result = index
    while bit < count:
        if k & bit:
            result = result + bit * (1 - 2 * lax.rem(index // bit, 2))
        bit *= 2
    return result


def plane_order(depth):
    if depth < 3:
        return list(range(depth))
    return [0, depth - 1] + list(range(1, depth - 1))


def kernel(
    ns, nt, src, rcv, cor, out, sbuf, rx, cbuf, csm, boxes, acc, r1, r2, nrm, hx, hz, rows, lap,
    in_sem, out_sem, rx_send, rx_recv, c_send, c_recv, c_local,
    s1_send, s1_recv, s2_send, s2_recv, row_send, row_recv, face_send, face_recv,
):
    depth, strip, width = nrm.shape
    spd, samples = src.shape[0], src.shape[1]
    box_rows = src.shape[3]
    halves = width // LANES
    order = plane_order(depth)
    shots = nt * spd
    block = min(box_rows, strip)
    per_strip = strip // block
    half_ns = ns // 2
    shot = lax.axis_index("shot")
    tile = lax.axis_index("tile")
    core = lax.rem(shot, 2)
    pair = shot // 2
    other = 1 - core

    barrier = pltpu.get_barrier_semaphore()
    for k in range(1, ns):
        pl.semaphore_signal(barrier, inc=1, device_id={"shot": lax.rem(shot + k, ns)})
    for k in range(1, nt):
        pl.semaphore_signal(barrier, inc=1, device_id={"tile": lax.rem(tile + k, nt)})

    for w, ref in enumerate((src, rcv)):
        for i in range(spd):
            for n in range(samples):
                pltpu.make_async_copy(ref.at[i, n], sbuf.at[:, w, i, n], in_sem).start()
    pltpu.make_async_copy(cor, cbuf.at[tile], c_recv).start()
    for p in order:
        for w, ref in enumerate((src, rcv)):
            pltpu.make_async_copy(ref.at[:, :, tile * depth + p], rx.at[p, tile, w], rx_recv.at[p]).start()
    pltpu.make_async_copy(sbuf, sbuf, in_sem).wait()

    pl.semaphore_wait(barrier, ns - 1 + nt - 1)

    for p in order:
        for k in range(nt - 1, 0, -1):
            to = partner(tile, k, nt)
            if p == order[0]:
                pltpu.make_async_remote_copy(
                    src_ref=cor, dst_ref=cbuf.at[tile], send_sem=c_send, recv_sem=c_recv, device_id={"tile": to}
                ).start()
            pltpu.make_async_remote_copy(
                src_ref=sbuf.at[to * depth + p],
                dst_ref=rx.at[p, tile],
                send_sem=rx_send.at[p],
                recv_sem=rx_recv.at[p],
                device_id={"tile": to},
            ).start()

    edges = (
        (shot < ns - 1, shot > 0, {"shot": lax.rem(shot + 1, ns)}),
        (shot > 0, shot < ns - 1, {"shot": lax.rem(shot + ns - 1, ns)}),
    )
    faces = (
        (tile < nt - 1, tile > 0, {"tile": lax.rem(tile + 1, nt)}, depth - 1),
        (tile > 0, tile < nt - 1, {"tile": lax.rem(tile + nt - 1, nt)}, 0),
    )
    for d in range(2):
        @pl.when(jnp.logical_not(edges[d][1]))
        def _(d=d):
            hx[d] = jnp.zeros((depth, 1, width), jnp.float32)

        @pl.when(jnp.logical_not(faces[d][1]))
        def _(d=d):
            hz[d] = jnp.zeros((strip, width), jnp.float32)

    def edge_copy(d, p):
        return pltpu.make_async_remote_copy(
            src_ref=rows.at[d, p], dst_ref=hx.at[d, p],
            send_sem=row_send.at[d, p], recv_sem=row_recv.at[d, p], device_id=edges[d][2],
        )

    def face_copy(d):
        return pltpu.make_async_remote_copy(
            src_ref=nrm.at[faces[d][3]], dst_ref=hz.at[d],
            send_sem=face_send.at[d], recv_sem=face_recv.at[d], device_id=faces[d][2],
        )

    zero = jnp.zeros((block, LANES), jnp.float32)

    def clear(s, carry):
        for q in range(2):
            for h in range(halves):
                boxes[s, q, h, pl.ds(0, block), :] = zero
                boxes[s, q, h, pl.ds(block + box_rows, block), :] = zero
        return carry

    lax.fori_loop(0, shots, clear, 0)

    pltpu.make_async_copy(cbuf, cbuf, c_recv).wait()
    to_scalar = pltpu.make_async_copy(cbuf, csm, c_local)
    to_scalar.start()
    to_scalar.wait()

    lane = lax.broadcasted_iota(jnp.int32, (box_rows, LANES), 1)

    def expand(p):
        def peer(t, carry):
            for i in range(spd):
                s = t * spd + i
                col = csm[t, i, 1]
                turn = lax.rem(col, LANES)
                image = jnp.zeros((box_rows, LANES), jnp.float32)
                light = image
                for n in range(samples):
                    wave = rx[p, t, 0, i, n].astype(jnp.float32)
                    back = rx[p, t, 1, i, n].astype(jnp.float32)
                    image = wave * back if n == 0 else image + wave * back
                    light = wave * wave if n == 0 else light + wave * wave
                image = pltpu.roll(image, turn, 1)
                light = pltpu.roll(light, turn, 1)
                for h in range(halves):
                    at = lane + (h * LANES - col)
                    inside = (at >= 0) & (at < LANES)
                    boxes[s, 0, h, pl.ds(block, box_rows), :] = jnp.where(inside, image, 0.0)
                    boxes[s, 1, h, pl.ds(block, box_rows), :] = jnp.where(inside, light, 0.0)
            return carry

        lax.fori_loop(0, nt, peer, 0)

    def place(p, parity):
        def one(n, carry):
            j = 2 * (n // per_strip) + parity
            base = lax.rem(n, per_strip) * block
            first = j * strip + base + block
            total = [[None] * halves for _ in range(2)]
            for s in range(shots):
                start = jnp.clip(first - csm[s // spd, s % spd, 0], 0, box_rows + block)
                for q in range(2):
                    for h in range(halves):
                        piece = boxes[s, q, h, pl.ds(start, block), :]
                        total[q][h] = piece if s == 0 else total[q][h] + piece
            for q in range(2):
                for h in range(halves):
                    acc[p, j, q, pl.ds(base, block), pl.ds(h * LANES, LANES)] = total[q][h]
            return carry

        lax.fori_loop(0, half_ns * per_strip, one, 0)

    def stage1(p):
        for i in range(half_ns):
            pltpu.make_async_remote_copy(
                src_ref=acc.at[p, 2 * i + other],
                dst_ref=r1.at[p, i],
                send_sem=s1_send.at[p],
                recv_sem=s1_recv.at[p],
                device_id={"shot": 2 * pair + other},
            ).start()

    def stage2(p):
        pltpu.make_async_copy(r1.at[p], r1.at[p], s1_recv.at[p]).wait()
        for k in range(1, half_ns):
            to = lax.rem(pair + k, half_ns)
            j = 2 * to + core
            acc[p, j] = acc[p, j] + r1[p, to]
            pltpu.make_async_remote_copy(
                src_ref=acc.at[p, j],
                dst_ref=r2.at[p, k - 1],
                send_sem=s2_send.at[p],
                recv_sem=s2_recv.at[p],
                device_id={"shot": j},
            ).start()

    def finish(p):
        pltpu.make_async_copy(r2.at[p], r2.at[p], s2_recv.at[p]).wait()
        image = acc[p, shot, 0] + r1[p, pair, 0]
        light = acc[p, shot, 1] + r1[p, pair, 1]
        for k in range(half_ns - 1):
            image = image + r2[p, k, 0]
            light = light + r2[p, k, 1]
        normal = image / (damping + light)
        nrm[p] = normal
        rows[0, p] = normal[strip - 1 :, :]
        rows[1, p] = normal[:1, :]
        for d in range(2):
            @pl.when(edges[d][0])
            def _(d=d):
                edge_copy(d, p).start()

            if p == faces[d][3]:
                @pl.when(faces[d][0])
                def _(d=d):
                    face_copy(d).start()

    row = lax.broadcasted_iota(jnp.int32, (strip, width), 0)
    column = lax.broadcasted_iota(jnp.int32, (strip, width), 1)

    def lateral(p):
        center = nrm[p]
        before = jnp.where(row == 0, 0.0, pltpu.roll(center, 1, 0))
        after = jnp.where(row == strip - 1, 0.0, pltpu.roll(center, strip - 1, 0))
        left = jnp.where(column == 0, 0.0, pltpu.roll(center, 1, 1))
        right = jnp.where(column == width - 1, 0.0, pltpu.roll(center, width - 1, 1))
        return before + after + left + right - 6.0 * center

    def wait_edges(p):
        for d in range(2):
            @pl.when(edges[d][1])
            def _(d=d):
                edge_copy(d, p).wait_recv()

    def add_edges(p):
        lap[p, pl.ds(0, 1), :] = lap[p, pl.ds(0, 1), :] + hx[0, p]
        lap[p, pl.ds(strip - 1, 1), :] = lap[p, pl.ds(strip - 1, 1), :] + hx[1, p]

    def emit(p):
        pltpu.make_async_copy(lap.at[p], out.at[p], out_sem.at[p]).start()

    for n, p in enumerate(order):
        pltpu.make_async_copy(rx.at[p], rx.at[p], rx_recv.at[p]).wait()
        expand(p)
        place(p, other)
        stage1(p)
        place(p, core)
        if n >= 1:
            stage2(order[n - 1])
        if n >= 2:
            finish(order[n - 2])
    last = order[-1]
    stage2(last)
    if depth >= 2:
        finish(order[-2])
    early = order[:-1]
    for d in range(2):
        if faces[d][3] != last:
            @pl.when(faces[d][1])
            def _(d=d):
                face_copy(d).wait_recv()
    for p in early:
        value = lateral(p)
        for near, d in ((p - 1, 0), (p + 1, 1)):
            if 0 <= near < depth:
                if near != last:
                    value = value + nrm[near]
            elif faces[d][3] != last:
                value = value + hz[d]
        lap[p] = value
        wait_edges(p)
        add_edges(p)
        if abs(p - last) > 1 and depth >= 3:
            emit(p)
    finish(last)
    for p in early:
        if abs(p - last) == 1:
            lap[p] = lap[p] + nrm[last]
            if depth >= 3:
                emit(p)
    value = lateral(last)
    for near in (last - 1, last + 1):
        if 0 <= near < depth:
            value = value + nrm[near]
    lap[last] = value
    for d in range(2):
        if faces[d][3] == last:
            @pl.when(faces[d][1])
            def _(d=d):
                face_copy(d).wait_recv()

    if depth < 3:
        for d, p in ((0, 0), (1, depth - 1)):
            if faces[d][3] == last or p == last:
                lap[p] = lap[p] + hz[d]
        for p in early:
            emit(p)
    wait_edges(last)
    add_edges(last)
    emit(last)
    for p in order:
        pltpu.make_async_copy(lap.at[p], out.at[p], out_sem.at[p]).wait()

    for d in range(2):
        @pl.when(edges[d][0])
        def _(d=d):
            for p in range(depth):
                edge_copy(d, p).wait_send()

        @pl.when(faces[d][0])
        def _(d=d):
            face_copy(d).wait_send()

    sent = cbuf.at[pl.ds(0, nt - 1)]
    pltpu.make_async_copy(sent, sent, c_send).wait()
    for p in range(depth):
        sent = rx.at[p, pl.ds(0, nt - 1)]
        pltpu.make_async_copy(sent, sent, rx_send.at[p]).wait()
        pltpu.make_async_copy(r1.at[p], r1.at[p], s1_send.at[p]).wait()
        pltpu.make_async_copy(r2.at[p], r2.at[p], s2_send.at[p]).wait()


def solution(mesh):
    ns, nt = mesh.shape["shot"], mesh.shape["tile"]

    def step(source, receiver, corners):
        spd, samples, full_depth, box_rows, box_cols = source.shape
        depth = full_depth // nt
        strip = X // ns
        block = min(box_rows, strip)
        half_ns = ns // 2
        vmem = pltpu.VMEM
        dma = pltpu.SemaphoreType.DMA
        f32 = jnp.float32
        return pl.pallas_call(
            functools.partial(kernel, ns, nt),
            out_shape=jax.ShapeDtypeStruct((depth, strip, Y), f32),
            in_specs=[pl.BlockSpec(memory_space=pl.ANY)] * 3,
            out_specs=pl.BlockSpec(memory_space=pl.ANY),
            scratch_shapes=[
                vmem((full_depth, 2, spd, samples, box_rows, box_cols), jnp.bfloat16),
                vmem((depth, nt, 2, spd, samples, box_rows, box_cols), jnp.bfloat16),
                vmem((nt, spd, 2), jnp.int32),
                pltpu.SMEM((nt, spd, 2), jnp.int32),
                vmem((nt * spd, 2, Y // LANES, box_rows + 2 * block, LANES), f32),
                vmem((depth, ns, 2, strip, Y), f32),
                vmem((depth, half_ns, 2, strip, Y), f32),
                vmem((depth, half_ns - 1, 2, strip, Y), f32),
                vmem((depth, strip, Y), f32),
                vmem((2, depth, 1, Y), f32),
                vmem((2, strip, Y), f32),
                vmem((2, depth, 1, Y), f32),
                vmem((depth, strip, Y), f32),
                dma,
                dma((depth,)),
                dma((depth,)),
                dma((depth,)),
                dma,
                dma,
                dma,
                dma((depth,)),
                dma((depth,)),
                dma((depth,)),
                dma((depth,)),
                dma((2, depth)),
                dma((2, depth)),
                dma((2,)),
                dma((2,)),
            ],
            compiler_params=pltpu.CompilerParams(
                collective_id=0, has_side_effects=True, vmem_limit_bytes=60 * 1024 * 1024
            ),
        )(source, receiver, corners)

    return jax.shard_map(
        step,
        mesh=mesh,
        in_specs=(
            P(("shot", "tile"), None, None, None, None),
            P(("shot", "tile"), None, None, None, None),
            P(("shot", "tile"), None),
        ),
        out_specs=P("tile", "shot", None),
        check_vma=False,
    )
```

```python
import functools

import jax
import jax.numpy as jnp
from jax import lax
from jax.experimental import pallas as pl
from jax.experimental.pallas import tpu as pltpu
from jax.sharding import PartitionSpec as P

X = 256
Y = 256
LANES = 128

damping = 1.0


def partner(index, k, count):
    if count & (count - 1):
        return lax.rem(index + k, count)
    bit = 1
    result = index
    while bit < count:
        if k & bit:
            result = result + bit * (1 - 2 * lax.rem(index // bit, 2))
        bit *= 2
    return result


def plane_order(depth):
    if depth < 3:
        return list(range(depth))
    return [0, depth - 1] + list(range(1, depth - 1))


def kernel(
    ns, nt, src, rcv, cor, out, sbuf, rx, cbuf, csm, boxes, acc, r1, r2, nrm, hx, hz, rows, lap,
    in_sem, out_sem, rx_send, rx_recv, c_send, c_recv, c_local,
    s1_send, s1_recv, s2_send, s2_recv, row_send, row_recv, face_send, face_recv, token,
):
    depth, strip, width = nrm.shape
    spd, samples = src.shape[0], src.shape[1]
    box_rows = src.shape[3]
    halves = width // LANES
    order = plane_order(depth)
    shots = nt * spd
    block = min(box_rows, strip)
    per_strip = strip // block
    half_ns = ns // 2
    shot = lax.axis_index("shot")
    tile = lax.axis_index("tile")
    core = lax.rem(shot, 2)
    pair = shot // 2
    other = 1 - core

    barrier = pltpu.get_barrier_semaphore()
    for k in range(1, ns):
        pl.semaphore_signal(barrier, inc=1, device_id={"shot": lax.rem(shot + k, ns)})
    place_at, side = tile // 2, lax.rem(tile, 2)
    places = nt // 2
    has_next, has_last = place_at < places - 1, place_at > 0
    after_me, before_me = lax.rem(tile + 2, nt), lax.rem(tile + nt - 2, nt)
    beside_me = tile + 1 - 2 * side
    pl.semaphore_signal(barrier, inc=1, device_id={"tile": beside_me})

    @pl.when(has_next)
    def _():
        pl.semaphore_signal(barrier, inc=1, device_id={"tile": after_me})

    @pl.when(has_last)
    def _():
        pl.semaphore_signal(barrier, inc=1, device_id={"tile": before_me})

    for w, ref in enumerate((src, rcv)):
        for i in range(spd):
            for n in range(samples):
                pltpu.make_async_copy(ref.at[i, n], sbuf.at[:, w, i, n], in_sem).start()
    pltpu.make_async_copy(cor, cbuf.at[tile], c_recv).start()
    for p in order:
        for w, ref in enumerate((src, rcv)):
            pltpu.make_async_copy(ref.at[:, :, tile * depth + p], rx.at[p, tile, w], rx_recv.at[p]).start()
    pltpu.make_async_copy(sbuf, sbuf, in_sem).wait()

    zero = jnp.zeros((block, LANES), jnp.float32)

    def clear(s, carry):
        for q in range(2):
            for h in range(halves):
                boxes[s, q, h, pl.ds(0, block), :] = zero
                boxes[s, q, h, pl.ds(block + box_rows, block), :] = zero
        return carry

    lax.fori_loop(0, shots, clear, 0)

    pl.semaphore_wait(barrier, ns + jnp.minimum(place_at, 1) + jnp.minimum(places - 1 - place_at, 1))

    @pl.when(has_last)
    def _():
        pl.semaphore_signal(token.at[0, 1], inc=1, device_id={"tile": before_me})

    @pl.when(has_next)
    def _():
        pl.semaphore_signal(token.at[1, 1], inc=1, device_id={"tile": after_me})

    def send_corner(to):
        pltpu.make_async_remote_copy(
            src_ref=cor, dst_ref=cbuf.at[tile], send_sem=c_send, recv_sem=c_recv, device_id={"tile": to}
        ).start()

    def send_plane(p, to):
        pltpu.make_async_remote_copy(
            src_ref=sbuf.at[to * depth + p],
            dst_ref=rx.at[p, tile],
            send_sem=rx_send.at[p],
            recv_sem=rx_recv.at[p],
            device_id={"tile": to},
        ).start()

    def send_all(to):
        send_corner(to)
        for p in order:
            send_plane(p, to)

    @pl.when(has_next)
    def _():
        send_all(after_me)

    @pl.when(has_last)
    def _():
        send_all(before_me)

    send_all(beside_me)

    for r in range(1, places):
        @pl.when(place_at + r < places)
        def _(r=r):
            pl.semaphore_wait(token.at[0, r], 1)

            @pl.when(has_last)
            def _():
                pl.semaphore_signal(token.at[0, r + 1], inc=1, device_id={"tile": before_me})

        @pl.when(place_at >= r)
        def _(r=r):
            pl.semaphore_wait(token.at[1, r], 1)

            @pl.when(has_next)
            def _():
                pl.semaphore_signal(token.at[1, r + 1], inc=1, device_id={"tile": after_me})

    for p in order:
        for k in range(nt - 1, 0, -1):
            to = partner(tile, k, nt)
            near = (to == beside_me) | ((to == after_me) & has_next) | ((to == before_me) & has_last)

            @pl.when(jnp.logical_not(near))
            def _(p=p, to=to):
                if p == order[0]:
                    send_corner(to)
                send_plane(p, to)

    edges = (
        (shot < ns - 1, shot > 0, {"shot": lax.rem(shot + 1, ns)}),
        (shot > 0, shot < ns - 1, {"shot": lax.rem(shot + ns - 1, ns)}),
    )
    faces = (
        (tile < nt - 1, tile > 0, {"tile": lax.rem(tile + 1, nt)}, depth - 1),
        (tile > 0, tile < nt - 1, {"tile": lax.rem(tile + nt - 1, nt)}, 0),
    )
    for d in range(2):
        @pl.when(jnp.logical_not(edges[d][1]))
        def _(d=d):
            hx[d] = jnp.zeros((depth, 1, width), jnp.float32)

        @pl.when(jnp.logical_not(faces[d][1]))
        def _(d=d):
            hz[d] = jnp.zeros((strip, width), jnp.float32)

    def edge_copy(d, p):
        return pltpu.make_async_remote_copy(
            src_ref=rows.at[d, p], dst_ref=hx.at[d, p],
            send_sem=row_send.at[d, p], recv_sem=row_recv.at[d, p], device_id=edges[d][2],
        )

    def face_copy(d):
        return pltpu.make_async_remote_copy(
            src_ref=nrm.at[faces[d][3]], dst_ref=hz.at[d],
            send_sem=face_send.at[d], recv_sem=face_recv.at[d], device_id=faces[d][2],
        )

    pltpu.make_async_copy(cbuf, cbuf, c_recv).wait()
    to_scalar = pltpu.make_async_copy(cbuf, csm, c_local)
    to_scalar.start()
    to_scalar.wait()

    lane = lax.broadcasted_iota(jnp.int32, (box_rows, LANES), 1)

    def expand(p):
        def peer(t, carry):
            for i in range(spd):
                s = t * spd + i
                col = csm[t, i, 1]
                turn = lax.rem(col, LANES)
                image = jnp.zeros((box_rows, LANES), jnp.float32)
                light = image
                for n in range(samples):
                    wave = rx[p, t, 0, i, n].astype(jnp.float32)
                    back = rx[p, t, 1, i, n].astype(jnp.float32)
                    image = wave * back if n == 0 else image + wave * back
                    light = wave * wave if n == 0 else light + wave * wave
                image = pltpu.roll(image, turn, 1)
                light = pltpu.roll(light, turn, 1)
                for h in range(halves):
                    at = lane + (h * LANES - col)
                    inside = (at >= 0) & (at < LANES)
                    boxes[s, 0, h, pl.ds(block, box_rows), :] = jnp.where(inside, image, 0.0)
                    boxes[s, 1, h, pl.ds(block, box_rows), :] = jnp.where(inside, light, 0.0)
            return carry

        lax.fori_loop(0, nt, peer, 0)

    def place(p, parity):
        def one(n, carry):
            j = 2 * (n // per_strip) + parity
            base = lax.rem(n, per_strip) * block
            first = j * strip + base + block
            total = [[None] * halves for _ in range(2)]
            for s in range(shots):
                start = jnp.clip(first - csm[s // spd, s % spd, 0], 0, box_rows + block)
                for q in range(2):
                    for h in range(halves):
                        piece = boxes[s, q, h, pl.ds(start, block), :]
                        total[q][h] = piece if s == 0 else total[q][h] + piece
            for q in range(2):
                for h in range(halves):
                    acc[p, j, q, pl.ds(base, block), pl.ds(h * LANES, LANES)] = total[q][h]
            return carry

        lax.fori_loop(0, half_ns * per_strip, one, 0)

    def stage1(p):
        for i in range(half_ns):
            pltpu.make_async_remote_copy(
                src_ref=acc.at[p, 2 * i + other],
                dst_ref=r1.at[p, i],
                send_sem=s1_send.at[p],
                recv_sem=s1_recv.at[p],
                device_id={"shot": 2 * pair + other},
            ).start()

    def stage2(p):
        pltpu.make_async_copy(r1.at[p], r1.at[p], s1_recv.at[p]).wait()
        for k in range(1, half_ns):
            to = lax.rem(pair + k, half_ns)
            j = 2 * to + core
            acc[p, j] = acc[p, j] + r1[p, to]
            pltpu.make_async_remote_copy(
                src_ref=acc.at[p, j],
                dst_ref=r2.at[p, k - 1],
                send_sem=s2_send.at[p],
                recv_sem=s2_recv.at[p],
                device_id={"shot": j},
            ).start()

    def finish(p):
        pltpu.make_async_copy(r2.at[p], r2.at[p], s2_recv.at[p]).wait()
        image = acc[p, shot, 0] + r1[p, pair, 0]
        light = acc[p, shot, 1] + r1[p, pair, 1]
        for k in range(half_ns - 1):
            image = image + r2[p, k, 0]
            light = light + r2[p, k, 1]
        normal = image / (damping + light)
        nrm[p] = normal
        rows[0, p] = normal[strip - 1 :, :]
        rows[1, p] = normal[:1, :]
        for d in range(2):
            @pl.when(edges[d][0])
            def _(d=d):
                edge_copy(d, p).start()

            if p == faces[d][3]:
                @pl.when(faces[d][0])
                def _(d=d):
                    face_copy(d).start()

    row = lax.broadcasted_iota(jnp.int32, (strip, width), 0)
    column = lax.broadcasted_iota(jnp.int32, (strip, width), 1)

    def lateral(p):
        center = nrm[p]
        before = jnp.where(row == 0, 0.0, pltpu.roll(center, 1, 0))
        after = jnp.where(row == strip - 1, 0.0, pltpu.roll(center, strip - 1, 0))
        left = jnp.where(column == 0, 0.0, pltpu.roll(center, 1, 1))
        right = jnp.where(column == width - 1, 0.0, pltpu.roll(center, width - 1, 1))
        return before + after + left + right - 6.0 * center

    def wait_edges(p):
        for d in range(2):
            @pl.when(edges[d][1])
            def _(d=d):
                edge_copy(d, p).wait_recv()

    def add_edges(p):
        lap[p, pl.ds(0, 1), :] = lap[p, pl.ds(0, 1), :] + hx[0, p]
        lap[p, pl.ds(strip - 1, 1), :] = lap[p, pl.ds(strip - 1, 1), :] + hx[1, p]

    def emit(p):
        pltpu.make_async_copy(lap.at[p], out.at[p], out_sem.at[p]).start()

    for n, p in enumerate(order):
        pltpu.make_async_copy(rx.at[p], rx.at[p], rx_recv.at[p]).wait()
        expand(p)
        place(p, other)
        stage1(p)
        place(p, core)
        if n >= 1:
            stage2(order[n - 1])
        if n >= 2:
            finish(order[n - 2])
    last = order[-1]
    stage2(last)
    if depth >= 2:
        finish(order[-2])
    early = order[:-1]
    for d in range(2):
        if faces[d][3] != last:
            @pl.when(faces[d][1])
            def _(d=d):
                face_copy(d).wait_recv()
    for p in early:
        value = lateral(p)
        for near, d in ((p - 1, 0), (p + 1, 1)):
            if 0 <= near < depth:
                if near != last:
                    value = value + nrm[near]
            elif faces[d][3] != last:
                value = value + hz[d]
        lap[p] = value
        wait_edges(p)
        add_edges(p)
        if abs(p - last) > 1 and depth >= 3:
            emit(p)
    finish(last)
    for p in early:
        if abs(p - last) == 1:
            lap[p] = lap[p] + nrm[last]
            if depth >= 3:
                emit(p)
    value = lateral(last)
    for near in (last - 1, last + 1):
        if 0 <= near < depth:
            value = value + nrm[near]
    lap[last] = value
    for d in range(2):
        if faces[d][3] == last:
            @pl.when(faces[d][1])
            def _(d=d):
                face_copy(d).wait_recv()

    if depth < 3:
        for d, p in ((0, 0), (1, depth - 1)):
            if faces[d][3] == last or p == last:
                lap[p] = lap[p] + hz[d]
        for p in early:
            emit(p)
    wait_edges(last)
    add_edges(last)
    emit(last)
    for p in order:
        pltpu.make_async_copy(lap.at[p], out.at[p], out_sem.at[p]).wait()

    for d in range(2):
        @pl.when(edges[d][0])
        def _(d=d):
            for p in range(depth):
                edge_copy(d, p).wait_send()

        @pl.when(faces[d][0])
        def _(d=d):
            face_copy(d).wait_send()

    sent = cbuf.at[pl.ds(0, nt - 1)]
    pltpu.make_async_copy(sent, sent, c_send).wait()
    for p in range(depth):
        sent = rx.at[p, pl.ds(0, nt - 1)]
        pltpu.make_async_copy(sent, sent, rx_send.at[p]).wait()
        pltpu.make_async_copy(r1.at[p], r1.at[p], s1_send.at[p]).wait()
        pltpu.make_async_copy(r2.at[p], r2.at[p], s2_send.at[p]).wait()


def solution(mesh):
    ns, nt = mesh.shape["shot"], mesh.shape["tile"]

    def step(source, receiver, corners):
        spd, samples, full_depth, box_rows, box_cols = source.shape
        depth = full_depth // nt
        strip = X // ns
        block = min(box_rows, strip)
        half_ns = ns // 2
        vmem = pltpu.VMEM
        dma = pltpu.SemaphoreType.DMA
        f32 = jnp.float32
        return pl.pallas_call(
            functools.partial(kernel, ns, nt),
            out_shape=jax.ShapeDtypeStruct((depth, strip, Y), f32),
            in_specs=[pl.BlockSpec(memory_space=pl.ANY)] * 3,
            out_specs=pl.BlockSpec(memory_space=pl.ANY),
            scratch_shapes=[
                vmem((full_depth, 2, spd, samples, box_rows, box_cols), jnp.bfloat16),
                vmem((depth, nt, 2, spd, samples, box_rows, box_cols), jnp.bfloat16),
                vmem((nt, spd, 2), jnp.int32),
                pltpu.SMEM((nt, spd, 2), jnp.int32),
                vmem((nt * spd, 2, Y // LANES, box_rows + 2 * block, LANES), f32),
                vmem((depth, ns, 2, strip, Y), f32),
                vmem((depth, half_ns, 2, strip, Y), f32),
                vmem((depth, half_ns - 1, 2, strip, Y), f32),
                vmem((depth, strip, Y), f32),
                vmem((2, depth, 1, Y), f32),
                vmem((2, strip, Y), f32),
                vmem((2, depth, 1, Y), f32),
                vmem((depth, strip, Y), f32),
                dma,
                dma((depth,)),
                dma((depth,)),
                dma((depth,)),
                dma,
                dma,
                dma,
                dma((depth,)),
                dma((depth,)),
                dma((depth,)),
                dma((depth,)),
                dma((2, depth)),
                dma((2, depth)),
                dma((2,)),
                dma((2,)),
                pltpu.SemaphoreType.REGULAR((2, nt // 2 + 1)),
            ],
            compiler_params=pltpu.CompilerParams(
                collective_id=0, has_side_effects=True, vmem_limit_bytes=60 * 1024 * 1024
            ),
        )(source, receiver, corners)

    return jax.shard_map(
        step,
        mesh=mesh,
        in_specs=(
            P(("shot", "tile"), None, None, None, None),
            P(("shot", "tile"), None, None, None, None),
            P(("shot", "tile"), None),
        ),
        out_specs=P("tile", "shot", None),
        check_vma=False,
    )
```

```python
import functools

import jax
import jax.numpy as jnp
from jax import lax
from jax.experimental import pallas as pl
from jax.experimental.pallas import tpu as pltpu
from jax.sharding import PartitionSpec as P

X = 256
Y = 256
LANES = 128

damping = 1.0


def partner(index, k, count):
    if count & (count - 1):
        return lax.rem(index + k, count)
    bit = 1
    result = index
    while bit < count:
        if k & bit:
            result = result + bit * (1 - 2 * lax.rem(index // bit, 2))
        bit *= 2
    return result


def plane_order(depth):
    if depth < 3:
        return list(range(depth))
    return [0, depth - 1] + list(range(1, depth - 1))


def kernel(
    ns, nt, src, rcv, cor, out, sbuf, rx, cbuf, csm, boxes, acc, r1, r2, nrm, hx, hz, rows, lap,
    in_sem, out_sem, rx_send, rx_recv, c_send, c_recv, c_local,
    s1_send, s1_recv, s2_send, s2_recv, row_send, row_recv, face_send, face_recv, token,
):
    depth, strip, width = nrm.shape
    spd, samples = src.shape[0], src.shape[1]
    box_rows = src.shape[3]
    halves = width // LANES
    order = plane_order(depth)
    shots = nt * spd
    block = min(box_rows, strip)
    per_strip = strip // block
    half_ns = ns // 2
    shot = lax.axis_index("shot")
    tile = lax.axis_index("tile")
    core = lax.rem(shot, 2)
    pair = shot // 2
    other = 1 - core

    barrier = pltpu.get_barrier_semaphore()
    for k in range(1, ns):
        pl.semaphore_signal(barrier, inc=1, device_id={"shot": lax.rem(shot + k, ns)})
    place_at, side = tile // 2, lax.rem(tile, 2)
    places = nt // 2
    has_next, has_last = place_at < places - 1, place_at > 0
    after_me, before_me = lax.rem(tile + 2, nt), lax.rem(tile + nt - 2, nt)
    beside_me = tile + 1 - 2 * side
    pl.semaphore_signal(barrier, inc=1, device_id={"tile": beside_me})

    @pl.when(has_next)
    def _():
        pl.semaphore_signal(barrier, inc=1, device_id={"tile": after_me})

    @pl.when(has_last)
    def _():
        pl.semaphore_signal(barrier, inc=1, device_id={"tile": before_me})

    for w, ref in enumerate((src, rcv)):
        for i in range(spd):
            for n in range(samples):
                pltpu.make_async_copy(ref.at[i, n], sbuf.at[:, w, i, n], in_sem).start()
    pltpu.make_async_copy(cor, cbuf.at[tile], c_recv).start()
    for p in order:
        for w, ref in enumerate((src, rcv)):
            pltpu.make_async_copy(ref.at[:, :, tile * depth + p], rx.at[p, tile, w], rx_recv.at[p]).start()
    pltpu.make_async_copy(sbuf, sbuf, in_sem).wait()

    zero = jnp.zeros((block, LANES), jnp.float32)

    def clear(s, carry):
        for q in range(2):
            for h in range(halves):
                boxes[s, q, h, pl.ds(0, block), :] = zero
                boxes[s, q, h, pl.ds(block + box_rows, block), :] = zero
        return carry

    lax.fori_loop(0, shots, clear, 0)

    pl.semaphore_wait(barrier, ns + jnp.minimum(place_at, 1) + jnp.minimum(places - 1 - place_at, 1))

    @pl.when(has_last)
    def _():
        pl.semaphore_signal(token.at[0, 1], inc=1, device_id={"tile": before_me})

    @pl.when(has_next)
    def _():
        pl.semaphore_signal(token.at[1, 1], inc=1, device_id={"tile": after_me})

    def send_corner(to):
        pltpu.make_async_remote_copy(
            src_ref=cor, dst_ref=cbuf.at[tile], send_sem=c_send, recv_sem=c_recv, device_id={"tile": to}
        ).start()

    def send_plane(p, to):
        pltpu.make_async_remote_copy(
            src_ref=sbuf.at[to * depth + p],
            dst_ref=rx.at[p, tile],
            send_sem=rx_send.at[p],
            recv_sem=rx_recv.at[p],
            device_id={"tile": to},
        ).start()

    def send_all(to):
        send_corner(to)
        send_plane(order[0], to)

    @pl.when(has_next)
    def _():
        send_all(after_me)

    @pl.when(has_last)
    def _():
        send_all(before_me)

    send_all(beside_me)

    for r in range(1, places):
        @pl.when(place_at + r < places)
        def _(r=r):
            pl.semaphore_wait(token.at[0, r], 1)

            @pl.when(has_last)
            def _():
                pl.semaphore_signal(token.at[0, r + 1], inc=1, device_id={"tile": before_me})

        @pl.when(place_at >= r)
        def _(r=r):
            pl.semaphore_wait(token.at[1, r], 1)

            @pl.when(has_next)
            def _():
                pl.semaphore_signal(token.at[1, r + 1], inc=1, device_id={"tile": after_me})

    for p in order:
        for k in range(nt - 1, 0, -1):
            to = partner(tile, k, nt)
            near = (to == beside_me) | ((to == after_me) & has_next) | ((to == before_me) & has_last)

            if p == order[0]:
                @pl.when(jnp.logical_not(near))
                def _(p=p, to=to):
                    send_corner(to)
                    send_plane(p, to)
            else:
                send_plane(p, to)

    edges = (
        (shot < ns - 1, shot > 0, {"shot": lax.rem(shot + 1, ns)}),
        (shot > 0, shot < ns - 1, {"shot": lax.rem(shot + ns - 1, ns)}),
    )
    faces = (
        (tile < nt - 1, tile > 0, {"tile": lax.rem(tile + 1, nt)}, depth - 1),
        (tile > 0, tile < nt - 1, {"tile": lax.rem(tile + nt - 1, nt)}, 0),
    )
    for d in range(2):
        @pl.when(jnp.logical_not(edges[d][1]))
        def _(d=d):
            hx[d] = jnp.zeros((depth, 1, width), jnp.float32)

        @pl.when(jnp.logical_not(faces[d][1]))
        def _(d=d):
            hz[d] = jnp.zeros((strip, width), jnp.float32)

    def edge_copy(d, p):
        return pltpu.make_async_remote_copy(
            src_ref=rows.at[d, p], dst_ref=hx.at[d, p],
            send_sem=row_send.at[d, p], recv_sem=row_recv.at[d, p], device_id=edges[d][2],
        )

    def face_copy(d):
        return pltpu.make_async_remote_copy(
            src_ref=nrm.at[faces[d][3]], dst_ref=hz.at[d],
            send_sem=face_send.at[d], recv_sem=face_recv.at[d], device_id=faces[d][2],
        )

    pltpu.make_async_copy(cbuf, cbuf, c_recv).wait()
    to_scalar = pltpu.make_async_copy(cbuf, csm, c_local)
    to_scalar.start()
    to_scalar.wait()

    lane = lax.broadcasted_iota(jnp.int32, (box_rows, LANES), 1)

    def expand(p):
        def peer(t, carry):
            for i in range(spd):
                s = t * spd + i
                col = csm[t, i, 1]
                turn = lax.rem(col, LANES)
                image = jnp.zeros((box_rows, LANES), jnp.float32)
                light = image
                for n in range(samples):
                    wave = rx[p, t, 0, i, n].astype(jnp.float32)
                    back = rx[p, t, 1, i, n].astype(jnp.float32)
                    image = wave * back if n == 0 else image + wave * back
                    light = wave * wave if n == 0 else light + wave * wave
                image = pltpu.roll(image, turn, 1)
                light = pltpu.roll(light, turn, 1)
                for h in range(halves):
                    at = lane + (h * LANES - col)
                    inside = (at >= 0) & (at < LANES)
                    boxes[s, 0, h, pl.ds(block, box_rows), :] = jnp.where(inside, image, 0.0)
                    boxes[s, 1, h, pl.ds(block, box_rows), :] = jnp.where(inside, light, 0.0)
            return carry

        lax.fori_loop(0, nt, peer, 0)

    def place(p, parity):
        def one(n, carry):
            j = 2 * (n // per_strip) + parity
            base = lax.rem(n, per_strip) * block
            first = j * strip + base + block
            total = [[None] * halves for _ in range(2)]
            for s in range(shots):
                start = jnp.clip(first - csm[s // spd, s % spd, 0], 0, box_rows + block)
                for q in range(2):
                    for h in range(halves):
                        piece = boxes[s, q, h, pl.ds(start, block), :]
                        total[q][h] = piece if s == 0 else total[q][h] + piece
            for q in range(2):
                for h in range(halves):
                    acc[p, j, q, pl.ds(base, block), pl.ds(h * LANES, LANES)] = total[q][h]
            return carry

        lax.fori_loop(0, half_ns * per_strip, one, 0)

    def stage1(p):
        for i in range(half_ns):
            pltpu.make_async_remote_copy(
                src_ref=acc.at[p, 2 * i + other],
                dst_ref=r1.at[p, i],
                send_sem=s1_send.at[p],
                recv_sem=s1_recv.at[p],
                device_id={"shot": 2 * pair + other},
            ).start()

    def stage2(p):
        pltpu.make_async_copy(r1.at[p], r1.at[p], s1_recv.at[p]).wait()
        for k in range(1, half_ns):
            to = lax.rem(pair + k, half_ns)
            j = 2 * to + core
            acc[p, j] = acc[p, j] + r1[p, to]
            pltpu.make_async_remote_copy(
                src_ref=acc.at[p, j],
                dst_ref=r2.at[p, k - 1],
                send_sem=s2_send.at[p],
                recv_sem=s2_recv.at[p],
                device_id={"shot": j},
            ).start()

    def finish(p):
        pltpu.make_async_copy(r2.at[p], r2.at[p], s2_recv.at[p]).wait()
        image = acc[p, shot, 0] + r1[p, pair, 0]
        light = acc[p, shot, 1] + r1[p, pair, 1]
        for k in range(half_ns - 1):
            image = image + r2[p, k, 0]
            light = light + r2[p, k, 1]
        normal = image / (damping + light)
        nrm[p] = normal
        rows[0, p] = normal[strip - 1 :, :]
        rows[1, p] = normal[:1, :]
        for d in range(2):
            @pl.when(edges[d][0])
            def _(d=d):
                edge_copy(d, p).start()

            if p == faces[d][3]:
                @pl.when(faces[d][0])
                def _(d=d):
                    face_copy(d).start()

    row = lax.broadcasted_iota(jnp.int32, (strip, width), 0)
    column = lax.broadcasted_iota(jnp.int32, (strip, width), 1)

    def lateral(p):
        center = nrm[p]
        before = jnp.where(row == 0, 0.0, pltpu.roll(center, 1, 0))
        after = jnp.where(row == strip - 1, 0.0, pltpu.roll(center, strip - 1, 0))
        left = jnp.where(column == 0, 0.0, pltpu.roll(center, 1, 1))
        right = jnp.where(column == width - 1, 0.0, pltpu.roll(center, width - 1, 1))
        return before + after + left + right - 6.0 * center

    def wait_edges(p):
        for d in range(2):
            @pl.when(edges[d][1])
            def _(d=d):
                edge_copy(d, p).wait_recv()

    def add_edges(p):
        lap[p, pl.ds(0, 1), :] = lap[p, pl.ds(0, 1), :] + hx[0, p]
        lap[p, pl.ds(strip - 1, 1), :] = lap[p, pl.ds(strip - 1, 1), :] + hx[1, p]

    def emit(p):
        pltpu.make_async_copy(lap.at[p], out.at[p], out_sem.at[p]).start()

    for n, p in enumerate(order):
        pltpu.make_async_copy(rx.at[p], rx.at[p], rx_recv.at[p]).wait()
        expand(p)
        place(p, other)
        stage1(p)
        place(p, core)
        if n >= 1:
            stage2(order[n - 1])
        if n >= 2:
            finish(order[n - 2])
    last = order[-1]
    stage2(last)
    if depth >= 2:
        finish(order[-2])
    early = order[:-1]
    for d in range(2):
        if faces[d][3] != last:
            @pl.when(faces[d][1])
            def _(d=d):
                face_copy(d).wait_recv()
    for p in early:
        value = lateral(p)
        for near, d in ((p - 1, 0), (p + 1, 1)):
            if 0 <= near < depth:
                if near != last:
                    value = value + nrm[near]
            elif faces[d][3] != last:
                value = value + hz[d]
        lap[p] = value
        wait_edges(p)
        add_edges(p)
        if abs(p - last) > 1 and depth >= 3:
            emit(p)
    finish(last)
    for p in early:
        if abs(p - last) == 1:
            lap[p] = lap[p] + nrm[last]
            if depth >= 3:
                emit(p)
    value = lateral(last)
    for near in (last - 1, last + 1):
        if 0 <= near < depth:
            value = value + nrm[near]
    lap[last] = value
    for d in range(2):
        if faces[d][3] == last:
            @pl.when(faces[d][1])
            def _(d=d):
                face_copy(d).wait_recv()

    if depth < 3:
        for d, p in ((0, 0), (1, depth - 1)):
            if faces[d][3] == last or p == last:
                lap[p] = lap[p] + hz[d]
        for p in early:
            emit(p)
    wait_edges(last)
    add_edges(last)
    emit(last)
    for p in order:
        pltpu.make_async_copy(lap.at[p], out.at[p], out_sem.at[p]).wait()

    for d in range(2):
        @pl.when(edges[d][0])
        def _(d=d):
            for p in range(depth):
                edge_copy(d, p).wait_send()

        @pl.when(faces[d][0])
        def _(d=d):
            face_copy(d).wait_send()

    sent = cbuf.at[pl.ds(0, nt - 1)]
    pltpu.make_async_copy(sent, sent, c_send).wait()
    for p in range(depth):
        sent = rx.at[p, pl.ds(0, nt - 1)]
        pltpu.make_async_copy(sent, sent, rx_send.at[p]).wait()
        pltpu.make_async_copy(r1.at[p], r1.at[p], s1_send.at[p]).wait()
        pltpu.make_async_copy(r2.at[p], r2.at[p], s2_send.at[p]).wait()


def solution(mesh):
    ns, nt = mesh.shape["shot"], mesh.shape["tile"]

    def step(source, receiver, corners):
        spd, samples, full_depth, box_rows, box_cols = source.shape
        depth = full_depth // nt
        strip = X // ns
        block = min(box_rows, strip)
        half_ns = ns // 2
        vmem = pltpu.VMEM
        dma = pltpu.SemaphoreType.DMA
        f32 = jnp.float32
        return pl.pallas_call(
            functools.partial(kernel, ns, nt),
            out_shape=jax.ShapeDtypeStruct((depth, strip, Y), f32),
            in_specs=[pl.BlockSpec(memory_space=pl.ANY)] * 3,
            out_specs=pl.BlockSpec(memory_space=pl.ANY),
            scratch_shapes=[
                vmem((full_depth, 2, spd, samples, box_rows, box_cols), jnp.bfloat16),
                vmem((depth, nt, 2, spd, samples, box_rows, box_cols), jnp.bfloat16),
                vmem((nt, spd, 2), jnp.int32),
                pltpu.SMEM((nt, spd, 2), jnp.int32),
                vmem((nt * spd, 2, Y // LANES, box_rows + 2 * block, LANES), f32),
                vmem((depth, ns, 2, strip, Y), f32),
                vmem((depth, half_ns, 2, strip, Y), f32),
                vmem((depth, half_ns - 1, 2, strip, Y), f32),
                vmem((depth, strip, Y), f32),
                vmem((2, depth, 1, Y), f32),
                vmem((2, strip, Y), f32),
                vmem((2, depth, 1, Y), f32),
                vmem((depth, strip, Y), f32),
                dma,
                dma((depth,)),
                dma((depth,)),
                dma((depth,)),
                dma,
                dma,
                dma,
                dma((depth,)),
                dma((depth,)),
                dma((depth,)),
                dma((depth,)),
                dma((2, depth)),
                dma((2, depth)),
                dma((2,)),
                dma((2,)),
                pltpu.SemaphoreType.REGULAR((2, nt // 2 + 1)),
            ],
            compiler_params=pltpu.CompilerParams(
                collective_id=0, has_side_effects=True, vmem_limit_bytes=60 * 1024 * 1024
            ),
        )(source, receiver, corners)

    return jax.shard_map(
        step,
        mesh=mesh,
        in_specs=(
            P(("shot", "tile"), None, None, None, None),
            P(("shot", "tile"), None, None, None, None),
            P(("shot", "tile"), None),
        ),
        out_specs=P("tile", "shot", None),
        check_vma=False,
    )
```
